32 devices in a mesh: grp: 2 (over x), blk: 16 (over z, y, core).
Axes of the slice: x: 2, y: 2, z: 4, core: 2. Of those that a mesh axis runs over, the one named last changes fastest.
Arguments:
- params: bfloat16 [2, 7168, 4096], P('grp', 'blk'), may hold values from -0.0625 to 0.0625
- tracker: bfloat16 [2, 7168, 4096], P('grp', 'blk'), may hold values from -0.29882812 to 0.29882812
- hidden: bfloat16 [256, 7168], P('grp', 'blk'), may hold values from -6 to 6
- target: bfloat16 [256, 4096], P('grp'), may hold values from -6 to 6
Outputs:
- params_next: bfloat16 [2, 7168, 4096], P('grp', 'blk')
- tracker_next: bfloat16 [2, 7168, 4096], P('grp', 'blk')
The draws below stay inside these ranges and needn't reach their ends.
All inputs are finite; a program needn't handle non-finite values.
Results may differ from the reference program's by a relative error of at most 0.01.
Values may be sent and summed in bfloat16 or wider, within the bound.
A program may use at most 192 MiB of HBM per device.

```python
import jax
import jax.numpy as jnp
from jax import lax

D = 4096
FF_WIN = 7168
TOK = 128
ALL_TOK = 256
N_GRP = 2


def levels(rng, extent, split, smallest, largest):
    def one(position, parts):
        draws = jax.random.uniform(jax.random.fold_in(jax.random.fold_in(rng, 6), position), (parts,), jnp.float32, smallest / len(split), largest / len(split))
        return jnp.repeat(jnp.exp(draws), extent[position] // parts).reshape((-1,) + (1,) * (len(extent) - position - 1))

    loudness = one(*split[0])
    for cut in split[1:]:
        loudness = loudness * one(*cut)
    return loudness


def noise(key, shape, width, bound, split=(), dtype=jnp.bfloat16):
    gain = levels(key, shape, split, -0.22, 0.18) if split else 1.0
    entries = jax.random.normal(key, shape, jnp.float32) * width * gain
    return jnp.minimum(jnp.maximum(entries, -bound), bound).astype(dtype)


def setup_inputs(seed: int = 0) -> dict:
    key_of = jax.random.split(jax.random.key(seed), 5)
    return {
        "params": noise(key_of[0], (N_GRP, FF_WIN, D), FF_WIN ** -0.5, 0.0625, ((0, 2), (1, 16))),
        "tracker": noise(key_of[1], (N_GRP, FF_WIN, D), 0.05, 0.29882812, ((0, 2), (1, 16))),
        "hidden": noise(key_of[2], (ALL_TOK, FF_WIN), 1.0, 6.0, ((0, 2), (1, 16))),
        "target": noise(key_of[3], (ALL_TOK, D), 1.0, 6.0, ((0, 2),)),
    }


step_size = 0.05


def mix(value):
    count = value.shape[0]
    zero_row = jnp.zeros_like(value[:1])
    left = jnp.concatenate([zero_row, value[:-1]], 0)
    right = jnp.concatenate([value[1:], zero_row], 0)
    place = jnp.arange(count)
    has_left = (place > 0).astype(jnp.float32)[:, None, None]
    has_right = (place < count - 1).astype(jnp.float32)[:, None, None]
    return value + has_left * (left - value) / 3.0 + has_right * (right - value) / 3.0


def gradient(weights, hidden_rows, target_rows):
    output = jnp.dot(hidden_rows, weights, preferred_element_type=jnp.float32)
    resid = jnp.tanh(output - target_rows.astype(jnp.float32)).astype(jnp.bfloat16)
    total = lax.dot_general(hidden_rows, resid, (((0,), (0,)), ((), ())), preferred_element_type=jnp.float32)
    return total / TOK


def reference(params, tracker, hidden, target):
    groups = params.shape[0]
    olds = []
    for replica in range(groups):
        olds.append(gradient(params[replica], hidden[replica * TOK:(replica + 1) * TOK], target[replica * TOK:(replica + 1) * TOK]))
    params_next = (mix(mix(params.astype(jnp.float32))) - step_size * tracker.astype(jnp.float32)).astype(jnp.bfloat16)
    mixed_tracker = mix(mix(tracker.astype(jnp.float32)))
    outcome = []
    for replica in range(groups):
        fresh = gradient(params_next[replica], hidden[replica * TOK:(replica + 1) * TOK], target[replica * TOK:(replica + 1) * TOK])
        outcome.append(mixed_tracker[replica] + fresh - olds[replica])
    tracker_next = jnp.stack(outcome).astype(jnp.bfloat16)
    return params_next, tracker_next
```

```python
import jax
import jax.numpy as jnp
from jax import lax
from jax.sharding import PartitionSpec as P

step_size = 0.05


def mix_weights(position, groups):
    def has(spot):
        return ((spot >= 0) & (spot < groups)).astype(jnp.float32)

    def row(spot):
        a, b = has(spot - 1) / 3.0, has(spot + 1) / 3.0
        return a, 1.0 - a - b, b

    here, before, after = row(position), row(position - 1), row(position + 1)
    return {
        -2: here[0] * before[0],
        -1: here[0] * before[1] + here[1] * here[0],
        0: here[1] * here[1] + here[0] * before[2] + here[2] * after[0],
        1: here[2] * after[1] + here[1] * here[2],
        2: here[2] * after[2],
    }


def from_replica(value, offset):
    size = lax.axis_size("grp")
    pairs = [(i, i - offset) for i in range(size) if 0 <= i - offset < size]
    return lax.ppermute(value, "grp", pairs)


def mixed(own, others, weights):
    total = weights[0] * own.astype(jnp.float32)
    for offset, value in others.items():
        total = total + weights[offset] * value.astype(jnp.float32)
    return total


def residual(weights, hidden, target):
    share = hidden.shape[0] // lax.axis_size("blk")
    own_output = lax.psum_scatter(
        jnp.dot(hidden, weights, preferred_element_type=jnp.float32),
        "blk",
        scatter_dimension=0,
        tiled=True,
    )
    own_target = lax.dynamic_slice_in_dim(target, lax.axis_index("blk") * share, share, 0)
    resid = jnp.tanh(own_output - own_target.astype(jnp.float32)).astype(jnp.bfloat16)
    return lax.all_gather(resid, "blk", axis=0, tiled=True)


def body(params, tracker, hidden, target):
    groups = lax.axis_size("grp")
    weights = mix_weights(lax.axis_index("grp"), groups)
    offsets = [o for o in (-2, -1, 1, 2) if abs(o) < groups]
    params, tracker = params[0], tracker[0]
    other_params = {o: from_replica(params, o) for o in offsets}
    other_tracker = {o: from_replica(tracker, o) for o in offsets}
    resid_old = residual(params, hidden, target)
    params_next = (
        mixed(params, other_params, weights) - step_size * tracker.astype(jnp.float32)
    ).astype(jnp.bfloat16)
    resid_new = residual(params_next, hidden, target)
    change = lax.dot_general(
        jnp.concatenate([hidden, -hidden], 0),
        jnp.concatenate([resid_new, resid_old], 0),
        (((0,), (0,)), ((), ())),
        preferred_element_type=jnp.float32,
    )
    tracker_next = (mixed(tracker, other_tracker, weights) + change / hidden.shape[0]).astype(jnp.bfloat16)
    return (params_next[None], tracker_next[None])


def solution(mesh):
    placed = (P("grp", "blk", None), P("grp", "blk", None), P("grp", "blk"), P("grp", None))
    return jax.shard_map(
        body,
        mesh=mesh,
        in_specs=placed,
        out_specs=(P("grp", "blk", None), P("grp", "blk", None)),
        check_vma=False,
    )
```

```python
import functools

import jax
import jax.numpy as jnp
from jax import lax
from jax.experimental import pallas as pl
from jax.experimental.pallas import tpu as pltpu
from jax.sharding import PartitionSpec as P

step_size = 0.05
MESH = pl.DeviceIdType.MESH


def mix_weights(position, groups):
    def has(spot):
        return ((spot >= 0) & (spot < groups)).astype(jnp.float32)

    def row(spot):
        a, b = has(spot - 1) / 3.0, has(spot + 1) / 3.0
        return a, 1.0 - a - b, b

    here, before, after = row(position), row(position - 1), row(position + 1)
    return {
        -2: here[0] * before[0],
        -1: here[0] * before[1] + here[1] * here[0],
        0: here[1] * here[1] + here[0] * before[2] + here[2] * after[0],
        1: here[2] * after[1] + here[1] * here[2],
        2: here[2] * after[2],
    }


def exchange(value, groups):
    if groups == 2:
        return {(-1, 1): lax.ppermute(value, "grp", [(0, 1), (1, 0)])}
    received = {}
    for offset in (-2, -1, 1, 2):
        pairs = [(i, i - offset) for i in range(groups) if 0 <= i - offset < groups]
        if pairs:
            received[(offset,)] = lax.ppermute(value, "grp", pairs)
    return received


def mixed(own, others, weights):
    total = weights[0] * own.astype(jnp.float32)
    for offsets, value in others.items():
        total = total + sum(weights[o] for o in offsets) * value.astype(jnp.float32)
    return total


def residual_kernel(n, part_ref, target_ref, out_ref, parts, send_sem, recv_sem, give_sem, take_sem):
    me = lax.axis_index("blk")
    peers = [lax.rem(me + k, n) for k in range(1, n)]

    barrier = pltpu.get_barrier_semaphore()
    for peer in peers:
        pl.semaphore_signal(barrier, inc=1, device_id={"blk": peer}, device_id_type=MESH)
    pl.semaphore_wait(barrier, n - 1)

    sums = []
    for k, peer in enumerate(peers):
        copy = pltpu.make_async_remote_copy(
            src_ref=part_ref.at[peer],
            dst_ref=parts.at[k],
            send_sem=send_sem.at[k],
            recv_sem=recv_sem.at[k],
            device_id={"blk": peer},
            device_id_type=MESH,
        )
        copy.start()
        sums.append(copy)
    total = part_ref[me].astype(jnp.float32) - target_ref[...].astype(jnp.float32)
    for k, copy in enumerate(sums):
        copy.wait_recv()
        total = total + parts[k].astype(jnp.float32)
    out_ref[me] = jnp.tanh(total).astype(jnp.bfloat16)

    spread = []
    for k, peer in enumerate(peers):
        copy = pltpu.make_async_remote_copy(
            src_ref=out_ref.at[me],
            dst_ref=out_ref.at[me],
            send_sem=give_sem.at[k],
            recv_sem=take_sem.at[k],
            device_id={"blk": peer},
            device_id_type=MESH,
        )
        copy.start()
        spread.append(copy)
    for copy in sums:
        copy.wait_send()
    for copy in spread:
        copy.wait()


def residual(output, own_target, n, which):
    tokens, width = output.shape
    share = tokens // n
    dma = pltpu.SemaphoreType.DMA((n - 1,))
    resid = pl.pallas_call(
        functools.partial(residual_kernel, n),
        out_shape=jax.ShapeDtypeStruct((n, share, width), jnp.bfloat16),
        in_specs=[pl.BlockSpec(memory_space=pltpu.VMEM)] * 2,
        out_specs=pl.BlockSpec(memory_space=pltpu.VMEM),
        scratch_shapes=[pltpu.VMEM((n - 1, share, width), jnp.bfloat16), dma, dma, dma, dma],
        compiler_params=pltpu.CompilerParams(collective_id=which, has_side_effects=True),
        cost_estimate=pl.CostEstimate(flops=0, bytes_accessed=100 * tokens * width, transcendentals=0),
        name="residual",
    )(output.astype(jnp.bfloat16).reshape(n, share, width), own_target)
    return resid.reshape(tokens, width)


def body(params, tracker, hidden, target):
    groups, n = lax.axis_size("grp"), lax.axis_size("blk")
    weights = mix_weights(lax.axis_index("grp"), groups)
    tokens = hidden.shape[0]
    share = tokens // n
    own_target = lax.dynamic_slice_in_dim(target, lax.axis_index("blk") * share, share, 0)
    params, tracker = params[0], tracker[0]
    other_params = exchange(params, groups)
    other_tracker = exchange(tracker, groups)
    output_old = jnp.dot(hidden, params, preferred_element_type=jnp.float32)
    resid_old = residual(output_old, own_target, n, 0)
    params_next = (
        mixed(params, other_params, weights) - step_size * tracker.astype(jnp.float32)
    ).astype(jnp.bfloat16)
    output_new = jnp.dot(hidden, params_next, preferred_element_type=jnp.float32)
    resid_new = residual(output_new, own_target, n, 1)
    change = lax.dot_general(
        jnp.concatenate([hidden, -hidden], 0),
        jnp.concatenate([resid_new, resid_old], 0),
        (((0,), (0,)), ((), ())),
        preferred_element_type=jnp.float32,
    )
    tracker_next = (mixed(tracker, other_tracker, weights) + change / tokens).astype(jnp.bfloat16)
    return (params_next[None], tracker_next[None])


def solution(mesh):
    placed = (P("grp", "blk", None), P("grp", "blk", None), P("grp", "blk"), P("grp", None))
    return jax.shard_map(
        body,
        mesh=mesh,
        in_specs=placed,
        out_specs=(P("grp", "blk", None), P("grp", "blk", None)),
        check_vma=False,
    )
```

```python
import functools

import jax
import jax.numpy as jnp
from jax import lax
from jax.experimental import pallas as pl
from jax.experimental.pallas import tpu as pltpu
from jax.sharding import PartitionSpec as P

step_size = 0.05
MESH = pl.DeviceIdType.MESH


def mix_weights(position, groups):
    def has(spot):
        return ((spot >= 0) & (spot < groups)).astype(jnp.float32)

    def row(spot):
        a, b = has(spot - 1) / 3.0, has(spot + 1) / 3.0
        return a, 1.0 - a - b, b

    here, before, after = row(position), row(position - 1), row(position + 1)
    return {
        -2: here[0] * before[0],
        -1: here[0] * before[1] + here[1] * here[0],
        0: here[1] * here[1] + here[0] * before[2] + here[2] * after[0],
        1: here[2] * after[1] + here[1] * here[2],
        2: here[2] * after[2],
    }


def exchange(value, groups):
    if groups == 2:
        return {(-1, 1): lax.ppermute(value, "grp", [(0, 1), (1, 0)])}
    received = {}
    for offset in (-2, -1, 1, 2):
        pairs = [(i, i - offset) for i in range(groups) if 0 <= i - offset < groups]
        if pairs:
            received[(offset,)] = lax.ppermute(value, "grp", pairs)
    return received


def mixed(own, others, weights):
    total = weights[0] * own.astype(jnp.float32)
    for offsets, value in others.items():
        total = total + sum(weights[o] for o in offsets) * value.astype(jnp.float32)
    return total


def residual_kernel(n, part_ref, target_ref, out_ref, parts, send_sem, recv_sem, give_sem, take_sem):
    me = lax.axis_index("blk")
    peers = [lax.rem(me + k, n) for k in range(1, n)]

    barrier = pltpu.get_barrier_semaphore()
    for peer in peers:
        pl.semaphore_signal(barrier, inc=1, device_id={"blk": peer}, device_id_type=MESH)
    pl.semaphore_wait(barrier, n - 1)

    sums = []
    for k, peer in enumerate(peers):
        copy = pltpu.make_async_remote_copy(
            src_ref=part_ref.at[peer],
            dst_ref=parts.at[k],
            send_sem=send_sem.at[k],
            recv_sem=recv_sem.at[k],
            device_id={"blk": peer},
            device_id_type=MESH,
        )
        copy.start()
        sums.append(copy)
    total = part_ref[me].astype(jnp.float32) - target_ref[...].astype(jnp.float32)
    for k, copy in enumerate(sums):
        copy.wait_recv()
        total = total + parts[k].astype(jnp.float32)
    out_ref[me] = jnp.tanh(total).astype(jnp.bfloat16)

    spread = []
    for k, peer in enumerate(peers):
        copy = pltpu.make_async_remote_copy(
            src_ref=out_ref.at[me],
            dst_ref=out_ref.at[me],
            send_sem=give_sem.at[k],
            recv_sem=take_sem.at[k],
            device_id={"blk": peer},
            device_id_type=MESH,
        )
        copy.start()
        spread.append(copy)
    for copy in sums:
        copy.wait_send()
    for copy in spread:
        copy.wait()


def residual(output, own_target, n, which):
    tokens, width = output.shape
    share = tokens // n
    dma = pltpu.SemaphoreType.DMA((n - 1,))
    resid = pl.pallas_call(
        functools.partial(residual_kernel, n),
        out_shape=jax.ShapeDtypeStruct((n, share, width), jnp.bfloat16),
        in_specs=[pl.BlockSpec(memory_space=pltpu.VMEM)] * 2,
        out_specs=pl.BlockSpec(memory_space=pltpu.VMEM),
        scratch_shapes=[pltpu.VMEM((n - 1, share, width), jnp.bfloat16), dma, dma, dma, dma],
        compiler_params=pltpu.CompilerParams(collective_id=which, has_side_effects=True),
        cost_estimate=pl.CostEstimate(flops=0, bytes_accessed=100 * tokens * width, transcendentals=0),
        name="residual",
    )(output.astype(jnp.bfloat16).reshape(n, share, width), own_target)
    return resid.reshape(tokens, width)


def add_kernel(count, weights_ref, base_ref, *refs):
    out_ref = refs[-1]
    total = base_ref[...]
    for i, other in enumerate(refs[:count]):
        total = total + weights_ref[i] * other[...].astype(jnp.float32)
    out_ref[...] = total.astype(out_ref.dtype)


def add_others(base, others, weights, first, block, into):
    rows, width = base.shape
    count = others[0].shape[0] // block
    start = first // block
    here = pl.BlockSpec((block, width), lambda i: (i + start, 0))
    there = pl.BlockSpec((block, width), lambda i: (i, 0))
    operands = [weights, base, *others]
    in_specs = [pl.BlockSpec(memory_space=pltpu.SMEM), here] + [there] * len(others)
    aliases = {}
    if into is not None:
        aliases = {len(operands): 0}
        operands.append(into)
        in_specs.append(pl.BlockSpec(memory_space=pl.ANY))
    return pl.pallas_call(
        functools.partial(add_kernel, len(others)),
        grid=(count,),
        out_shape=jax.ShapeDtypeStruct((rows, width), jnp.bfloat16),
        in_specs=in_specs,
        out_specs=here,
        input_output_aliases=aliases,
        compiler_params=pltpu.CompilerParams(dimension_semantics=("arbitrary",)),
        cost_estimate=pl.CostEstimate(
            flops=4 * count * block * width, bytes_accessed=8 * count * block * width, transcendentals=0
        ),
        name="add_others",
    )(*operands)


def body(params, tracker, hidden, target):
    groups, n = lax.axis_size("grp"), lax.axis_size("blk")
    weights = mix_weights(lax.axis_index("grp"), groups)
    tokens = hidden.shape[0]
    share = tokens // n
    own_target = lax.dynamic_slice_in_dim(target, lax.axis_index("blk") * share, share, 0)
    params, tracker = params[0], tracker[0]
    rows = params.shape[0]
    block = max(rows // 7 // 16, 1) * 16
    cuts = [(0, rows - block), (rows - block, rows)]
    other_params = exchange(params, groups)
    other_tracker = [exchange(tracker[lo:hi], groups) for lo, hi in cuts]
    output_old = jnp.dot(hidden, params, preferred_element_type=jnp.float32)
    resid_old = residual(output_old, own_target, n, 0)
    params_next = (
        mixed(params, other_params, weights) - step_size * tracker.astype(jnp.float32)
    ).astype(jnp.bfloat16)
    output_new = jnp.dot(hidden, params_next, preferred_element_type=jnp.float32)
    resid_new = residual(output_new, own_target, n, 1)
    change = lax.dot_general(
        jnp.concatenate([hidden, -hidden], 0),
        jnp.concatenate([resid_new, resid_old], 0),
        (((0,), (0,)), ((), ())),
        preferred_element_type=jnp.float32,
    )
    base = weights[0] * tracker.astype(jnp.float32) + change / tokens
    tracker_next = None
    for (lo, _), received in zip(cuts, other_tracker):
        gains = jnp.stack([sum(weights[o] for o in offsets) for offsets in received])
        tracker_next = add_others(base, list(received.values()), gains, lo, block, tracker_next)
    return (params_next[None], tracker_next[None])


def solution(mesh):
    placed = (P("grp", "blk", None), P("grp", "blk", None), P("grp", "blk"), P("grp", None))
    return jax.shard_map(
        body,
        mesh=mesh,
        in_specs=placed,
        out_specs=(P("grp", "blk", None), P("grp", "blk", None)),
        check_vma=False,
    )
```

```python
import functools

import jax
import jax.numpy as jnp
from jax import lax
from jax.experimental import pallas as pl
from jax.experimental.pallas import tpu as pltpu
from jax.sharding import PartitionSpec as P

step_size = 0.05
MESH = pl.DeviceIdType.MESH


def mix_weights(position, groups):
    def has(spot):
        return ((spot >= 0) & (spot < groups)).astype(jnp.float32)

    def row(spot):
        a, b = has(spot - 1) / 3.0, has(spot + 1) / 3.0
        return a, 1.0 - a - b, b

    here, before, after = row(position), row(position - 1), row(position + 1)
    return {
        -2: here[0] * before[0],
        -1: here[0] * before[1] + here[1] * here[0],
        0: here[1] * here[1] + here[0] * before[2] + here[2] * after[0],
        1: here[2] * after[1] + here[1] * here[2],
        2: here[2] * after[2],
    }


def exchange(value, groups):
    if groups == 2:
        return {(-1, 1): lax.ppermute(value, "grp", [(0, 1), (1, 0)])}
    received = {}
    for offset in (-2, -1, 1, 2):
        pairs = [(i, i - offset) for i in range(groups) if 0 <= i - offset < groups]
        if pairs:
            received[(offset,)] = lax.ppermute(value, "grp", pairs)
    return received


def mixed(own, others, weights):
    total = weights[0] * own.astype(jnp.float32)
    for offsets, value in others.items():
        total = total + sum(weights[o] for o in offsets) * value.astype(jnp.float32)
    return total


PIECES = 4


def residual_kernel(
    z_size, part_ref, target_ref, out_ref, core_in, core_sum, y_in, y_sum, z_in, *sems
):
    (core_s, core_r, y_s, y_r, z_s, z_r, gz_s, gz_r, gy_s, gy_r, gc_s, gc_r) = sems
    me = lax.axis_index("blk")
    c = lax.rem(me, 2)
    y = lax.rem(lax.div(me, 2), 2)
    z = lax.div(me, 4)
    core_peer = z * 4 + y * 2 + (1 - c)
    y_peer = z * 4 + (1 - y) * 2 + c
    z_spots = [lax.rem(z + k, z_size) for k in range(1, z_size)]
    z_peers = [spot * 4 + y * 2 + c for spot in z_spots]
    width = target_ref.shape[-1] // PIECES
    columns = [pl.ds(q * width, width) for q in range(PIECES)]

    barrier = pltpu.get_barrier_semaphore()
    for peer in [core_peer, y_peer, *z_peers]:
        pl.semaphore_signal(barrier, inc=1, device_id={"blk": peer}, device_id_type=MESH)
    pl.semaphore_wait(barrier, z_size + 1)

    def send(src, dst, send_sem, recv_sem, peer):
        copy = pltpu.make_async_remote_copy(
            src_ref=src,
            dst_ref=dst,
            send_sem=send_sem,
            recv_sem=recv_sem,
            device_id={"blk": peer},
            device_id_type=MESH,
        )
        copy.start()
        return copy

    over_core = [
        send(part_ref.at[:, :, 1 - c, :, at], core_in.at[:, :, :, at], core_s.at[q], core_r.at[q], core_peer)
        for q, at in enumerate(columns)
    ]
    over_y = []
    for q, at in enumerate(columns):
        over_core[q].wait_recv()
        core_sum[:, :, :, at] = part_ref[:, :, c, :, at] + core_in[:, :, :, at]
        over_y.append(
            send(core_sum.at[:, 1 - y, :, at], y_in.at[:, :, at], y_s.at[q], y_r.at[q], y_peer)
        )
    over_z = []
    for q, at in enumerate(columns):
        over_y[q].wait_recv()
        y_sum[:, :, at] = core_sum[:, y, :, at] + y_in[:, :, at]
        over_z.append([
            send(y_sum.at[spot, :, at], z_in.at[k, :, at], z_s.at[q, k], z_r.at[q, k], z_peers[k])
            for k, spot in enumerate(z_spots)
        ])
    give_z = []
    for q, at in enumerate(columns):
        total = y_sum[z, :, at] - target_ref[:, at].astype(jnp.float32)
        for k, copy in enumerate(over_z[q]):
            copy.wait_recv()
            total = total + z_in[k, :, at]
        out_ref[z, y, c, :, at] = jnp.tanh(total).astype(jnp.bfloat16)
        mine = out_ref.at[z, y, c, :, at]
        give_z.append([
            send(mine, mine, gz_s.at[q, k], gz_r.at[q, k], peer) for k, peer in enumerate(z_peers)
        ])
    give_y = []
    for q, at in enumerate(columns):
        for copy in give_z[q]:
            copy.wait_recv()
        mine = out_ref.at[:, y, c, :, at]
        give_y.append(send(mine, mine, gy_s.at[q], gy_r.at[q], y_peer))
    give_core = []
    for q, at in enumerate(columns):
        give_y[q].wait_recv()
        mine = out_ref.at[:, :, c, :, at]
        give_core.append(send(mine, mine, gc_s.at[q], gc_r.at[q], core_peer))
    for copy in give_core:
        copy.wait_recv()
    for copy in [*over_core, *over_y, *sum(over_z, []), *sum(give_z, []), *give_y, *give_core]:
        copy.wait_send()


def residual(output, own_target, n, which):
    tokens, width = output.shape
    share, z_size = tokens // n, n // 4
    one = pltpu.SemaphoreType.DMA((PIECES,))
    many = pltpu.SemaphoreType.DMA((PIECES, z_size - 1))
    resid = pl.pallas_call(
        functools.partial(residual_kernel, z_size),
        out_shape=jax.ShapeDtypeStruct((z_size, 2, 2, share, width), jnp.bfloat16),
        in_specs=[pl.BlockSpec(memory_space=pltpu.VMEM)] * 2,
        out_specs=pl.BlockSpec(memory_space=pltpu.VMEM),
        scratch_shapes=[
            pltpu.VMEM((z_size, 2, share, width), jnp.float32),
            pltpu.VMEM((z_size, 2, share, width), jnp.float32),
            pltpu.VMEM((z_size, share, width), jnp.float32),
            pltpu.VMEM((z_size, share, width), jnp.float32),
            pltpu.VMEM((z_size - 1, share, width), jnp.float32),
            one, one, one, one, many, many, many, many, one, one, one, one,
        ],
        compiler_params=pltpu.CompilerParams(collective_id=which, has_side_effects=True),
        cost_estimate=pl.CostEstimate(flops=0, bytes_accessed=100 * tokens * width, transcendentals=0),
        name="residual",
    )(output.reshape(z_size, 2, 2, share, width), own_target)
    return resid.reshape(tokens, width)


def add_kernel(count, weights_ref, base_ref, *refs):
    out_ref = refs[-1]
    total = base_ref[...]
    for i, other in enumerate(refs[:count]):
        total = total + weights_ref[i] * other[...].astype(jnp.float32)
    out_ref[...] = total.astype(out_ref.dtype)


def add_others(base, others, weights, first, block, into):
    rows, width = base.shape
    count = others[0].shape[0] // block
    start = first // block
    here = pl.BlockSpec((block, width), lambda i: (i + start, 0))
    there = pl.BlockSpec((block, width), lambda i: (i, 0))
    operands = [weights, base, *others]
    in_specs = [pl.BlockSpec(memory_space=pltpu.SMEM), here] + [there] * len(others)
    aliases = {}
    if into is not None:
        aliases = {len(operands): 0}
        operands.append(into)
        in_specs.append(pl.BlockSpec(memory_space=pl.ANY))
    return pl.pallas_call(
        functools.partial(add_kernel, len(others)),
        grid=(count,),
        out_shape=jax.ShapeDtypeStruct((rows, width), jnp.bfloat16),
        in_specs=in_specs,
        out_specs=here,
        input_output_aliases=aliases,
        compiler_params=pltpu.CompilerParams(dimension_semantics=("arbitrary",)),
        cost_estimate=pl.CostEstimate(
            flops=4 * count * block * width, bytes_accessed=8 * count * block * width, transcendentals=0
        ),
        name="add_others",
    )(*operands)


def body(params, tracker, hidden, target):
    groups, n = lax.axis_size("grp"), lax.axis_size("blk")
    weights = mix_weights(lax.axis_index("grp"), groups)
    tokens = hidden.shape[0]
    share = tokens // n
    own_target = lax.dynamic_slice_in_dim(target, lax.axis_index("blk") * share, share, 0)
    params, tracker = params[0], tracker[0]
    rows = params.shape[0]
    block = max(rows // 7 // 16, 1) * 16
    cuts = [(0, rows - block), (rows - block, rows)]
    other_params = exchange(params, groups)
    other_tracker = [exchange(tracker[lo:hi], groups) for lo, hi in cuts]
    output_old = jnp.dot(hidden, params, preferred_element_type=jnp.float32)
    resid_old = residual(output_old, own_target, n, 0)
    params_next = (
        mixed(params, other_params, weights) - step_size * tracker.astype(jnp.float32)
    ).astype(jnp.bfloat16)
    output_new = jnp.dot(hidden, params_next, preferred_element_type=jnp.float32)
    resid_new = residual(output_new, own_target, n, 1)
    change = lax.dot_general(
        jnp.concatenate([hidden, -hidden], 0),
        jnp.concatenate([resid_new, resid_old], 0),
        (((0,), (0,)), ((), ())),
        preferred_element_type=jnp.float32,
    )
    base = weights[0] * tracker.astype(jnp.float32) + change / tokens
    tracker_next = None
    for (lo, _), received in zip(cuts, other_tracker):
        gains = jnp.stack([sum(weights[o] for o in offsets) for offsets in received])
        tracker_next = add_others(base, list(received.values()), gains, lo, block, tracker_next)
    return (params_next[None], tracker_next[None])


def solution(mesh):
    placed = (P("grp", "blk", None), P("grp", "blk", None), P("grp", "blk"), P("grp", None))
    return jax.shard_map(
        body,
        mesh=mesh,
        in_specs=placed,
        out_specs=(P("grp", "blk", None), P("grp", "blk", None)),
        check_vma=False,
    )
```

```python
import functools

import jax
import jax.numpy as jnp
from jax import lax
from jax.experimental import pallas as pl
from jax.experimental.pallas import tpu as pltpu
from jax.sharding import PartitionSpec as P

step_size = 0.05
MESH = pl.DeviceIdType.MESH


def mix_weights(position, groups):
    def has(spot):
        return ((spot >= 0) & (spot < groups)).astype(jnp.float32)

    def row(spot):
        a, b = has(spot - 1) / 3.0, has(spot + 1) / 3.0
        return a, 1.0 - a - b, b

    here, before, after = row(position), row(position - 1), row(position + 1)
    return {
        -2: here[0] * before[0],
        -1: here[0] * before[1] + here[1] * here[0],
        0: here[1] * here[1] + here[0] * before[2] + here[2] * after[0],
        1: here[2] * after[1] + here[1] * here[2],
        2: here[2] * after[2],
    }


def exchange(value, groups):
    if groups == 2:
        return {(-1, 1): lax.ppermute(value, "grp", [(0, 1), (1, 0)])}
    received = {}
    for offset in (-2, -1, 1, 2):
        pairs = [(i, i - offset) for i in range(groups) if 0 <= i - offset < groups]
        if pairs:
            received[(offset,)] = lax.ppermute(value, "grp", pairs)
    return received


def mixed(own, others, weights):
    total = weights[0] * own.astype(jnp.float32)
    for offsets, value in others.items():
        total = total + sum(weights[o] for o in offsets) * value.astype(jnp.float32)
    return total


PIECES = 4


def residual_kernel(
    z_size, part_ref, target_ref, out_ref, core_in, core_sum, y_in, y_sum, z_in, *sems
):
    (core_s, core_r, y_s, y_r, z_s, z_r, gz_s, gz_r, gy_s, gy_r, gc_s, gc_r) = sems
    me = lax.axis_index("blk")
    c = lax.rem(me, 2)
    y = lax.rem(lax.div(me, 2), 2)
    z = lax.div(me, 4)
    core_peer = z * 4 + y * 2 + (1 - c)
    y_peer = z * 4 + (1 - y) * 2 + c
    z_spots = [lax.rem(z + k, z_size) for k in range(1, z_size)]
    z_peers = [spot * 4 + y * 2 + c for spot in z_spots]
    width = target_ref.shape[-1] // PIECES
    columns = [pl.ds(q * width, width) for q in range(PIECES)]

    barrier = pltpu.get_barrier_semaphore()
    for peer in [core_peer, y_peer, *z_peers]:
        pl.semaphore_signal(barrier, inc=1, device_id={"blk": peer}, device_id_type=MESH)
    pl.semaphore_wait(barrier, z_size + 1)

    def send(src, dst, send_sem, recv_sem, peer):
        copy = pltpu.make_async_remote_copy(
            src_ref=src,
            dst_ref=dst,
            send_sem=send_sem,
            recv_sem=recv_sem,
            device_id={"blk": peer},
            device_id_type=MESH,
        )
        copy.start()
        return copy

    over_core = [
        send(part_ref.at[:, :, 1 - c, :, at], core_in.at[:, :, :, at], core_s.at[q], core_r.at[q], core_peer)
        for q, at in enumerate(columns)
    ]
    over_y = []
    for q, at in enumerate(columns):
        over_core[q].wait_recv()
        core_sum[:, :, :, at] = part_ref[:, :, c, :, at] + core_in[:, :, :, at]
        over_y.append(
            send(core_sum.at[:, 1 - y, :, at], y_in.at[:, :, at], y_s.at[q], y_r.at[q], y_peer)
        )
    over_z = []
    for q, at in enumerate(columns):
        over_y[q].wait_recv()
        y_sum[:, :, at] = core_sum[:, y, :, at] + y_in[:, :, at]
        over_z.append([
            send(y_sum.at[spot, :, at], z_in.at[k, :, at], z_s.at[q, k], z_r.at[q, k], z_peers[k])
            for k, spot in enumerate(z_spots)
        ])
    give_z = []
    for q, at in enumerate(columns):
        total = y_sum[z, :, at] - target_ref[:, at].astype(jnp.float32)
        for k, copy in enumerate(over_z[q]):
            copy.wait_recv()
            total = total + z_in[k, :, at]
        out_ref[z, y, c, :, at] = jnp.tanh(total).astype(jnp.bfloat16)
        mine = out_ref.at[z, y, c, :, at]
        give_z.append([
            send(mine, mine, gz_s.at[q, k], gz_r.at[q, k], peer) for k, peer in enumerate(z_peers)
        ])
    give_y = []
    for q, at in enumerate(columns):
        for copy in give_z[q]:
            copy.wait_recv()
        mine = out_ref.at[:, y, c, :, at]
        give_y.append(send(mine, mine, gy_s.at[q], gy_r.at[q], y_peer))
    give_core = []
    for q, at in enumerate(columns):
        give_y[q].wait_recv()
        mine = out_ref.at[:, :, c, :, at]
        give_core.append(send(mine, mine, gc_s.at[q], gc_r.at[q], core_peer))
    for copy in give_core:
        copy.wait_recv()
    for copy in [*over_core, *over_y, *sum(over_z, []), *sum(give_z, []), *give_y, *give_core]:
        copy.wait_send()


def residual(output, own_target, n, which):
    tokens, width = output.shape
    share, z_size = tokens // n, n // 4
    one = pltpu.SemaphoreType.DMA((PIECES,))
    many = pltpu.SemaphoreType.DMA((PIECES, z_size - 1))
    resid = pl.pallas_call(
        functools.partial(residual_kernel, z_size),
        out_shape=jax.ShapeDtypeStruct((z_size, 2, 2, share, width), jnp.bfloat16),
        in_specs=[pl.BlockSpec(memory_space=pltpu.VMEM)] * 2,
        out_specs=pl.BlockSpec(memory_space=pltpu.VMEM),
        scratch_shapes=[
            pltpu.VMEM((z_size, 2, share, width), jnp.float32),
            pltpu.VMEM((z_size, 2, share, width), jnp.float32),
            pltpu.VMEM((z_size, share, width), jnp.float32),
            pltpu.VMEM((z_size, share, width), jnp.float32),
            pltpu.VMEM((z_size - 1, share, width), jnp.float32),
            one, one, one, one, many, many, many, many, one, one, one, one,
        ],
        compiler_params=pltpu.CompilerParams(collective_id=which, has_side_effects=True),
        cost_estimate=pl.CostEstimate(flops=0, bytes_accessed=100 * tokens * width, transcendentals=0),
        name="residual",
    )(output.reshape(z_size, 2, 2, share, width), own_target)
    return resid.reshape(tokens, width)


def add_kernel(count, weights_ref, base_ref, *refs):
    out_ref = refs[-1]
    total = base_ref[...]
    for i, other in enumerate(refs[:count]):
        total = total + weights_ref[i] * other[...].astype(jnp.float32)
    out_ref[...] = total.astype(out_ref.dtype)


def add_others(base, others, weights, block):
    rows, width = base.shape
    count = others[0].shape[0] // block
    here = pl.BlockSpec((block, width), lambda i: (i, 0))
    return pl.pallas_call(
        functools.partial(add_kernel, len(others)),
        grid=(count,),
        out_shape=jax.ShapeDtypeStruct((rows, width), jnp.bfloat16),
        in_specs=[pl.BlockSpec(memory_space=pltpu.SMEM), here] + [here] * len(others),
        out_specs=here,
        compiler_params=pltpu.CompilerParams(dimension_semantics=("arbitrary",)),
        cost_estimate=pl.CostEstimate(
            flops=4 * count * block * width, bytes_accessed=8 * count * block * width, transcendentals=0
        ),
        name="add_others",
    )(weights, base, *others)


def body(params, tracker, hidden, target):
    groups, n = lax.axis_size("grp"), lax.axis_size("blk")
    weights = mix_weights(lax.axis_index("grp"), groups)
    tokens = hidden.shape[0]
    share = tokens // n
    own_target = lax.dynamic_slice_in_dim(target, lax.axis_index("blk") * share, share, 0)
    params, tracker = params[0], tracker[0]
    rows = params.shape[0]
    block = max(rows // 14 // 16, 1) * 16
    cuts = [(0, rows - 4 * block), (rows - 4 * block, rows - block), (rows - block, rows)]
    other_params = exchange(params, groups)
    other_tracker = [exchange(tracker[lo:hi], groups) for lo, hi in cuts]
    output_old = jnp.dot(hidden, params, preferred_element_type=jnp.float32)
    resid_old = residual(output_old, own_target, n, 0)
    params_next = (
        mixed(params, other_params, weights) - step_size * tracker.astype(jnp.float32)
    ).astype(jnp.bfloat16)
    output_new = jnp.dot(hidden, params_next, preferred_element_type=jnp.float32)
    resid_new = residual(output_new, own_target, n, 1)
    change = lax.dot_general(
        jnp.concatenate([hidden, -hidden], 0),
        jnp.concatenate([resid_new, resid_old], 0),
        (((0,), (0,)), ((), ())),
        preferred_element_type=jnp.float32,
    )
    base = weights[0] * tracker.astype(jnp.float32) + change / tokens
    gains = jnp.stack([sum(weights[o] for o in offsets) for offsets in other_tracker[0]])
    first = list(other_tracker[0].values())
    step = next(size for size in (4 * block, 2 * block, block) if first[0].shape[0] % size == 0)
    tracker_next = add_others(base, first, gains, step)
    for (lo, hi), received in zip(cuts[1:], other_tracker[1:]):
        piece = base[lo:hi]
        for gain, value in zip(gains, received.values()):
            piece = piece + gain * value.astype(jnp.float32)
        tracker_next = lax.dynamic_update_slice(tracker_next, piece.astype(jnp.bfloat16), (lo, 0))
    return (params_next[None], tracker_next[None])


def solution(mesh):
    placed = (P("grp", "blk", None), P("grp", "blk", None), P("grp", "blk"), P("grp", None))
    return jax.shard_map(
        body,
        mesh=mesh,
        in_specs=placed,
        out_specs=(P("grp", "blk", None), P("grp", "blk", None)),
        check_vma=False,
    )
```

```python
import functools

import jax
import jax.numpy as jnp
from jax import lax
from jax.experimental import pallas as pl
from jax.experimental.pallas import tpu as pltpu
from jax.sharding import PartitionSpec as P

step_size = 0.05
MESH = pl.DeviceIdType.MESH


def mix_weights(position, groups):
    def has(spot):
        return ((spot >= 0) & (spot < groups)).astype(jnp.float32)

    def row(spot):
        a, b = has(spot - 1) / 3.0, has(spot + 1) / 3.0
        return a, 1.0 - a - b, b

    here, before, after = row(position), row(position - 1), row(position + 1)
    return {
        -2: here[0] * before[0],
        -1: here[0] * before[1] + here[1] * here[0],
        0: here[1] * here[1] + here[0] * before[2] + here[2] * after[0],
        1: here[2] * after[1] + here[1] * here[2],
        2: here[2] * after[2],
    }


def exchange(value, groups):
    if groups == 2:
        return {(-1, 1): lax.ppermute(value, "grp", [(0, 1), (1, 0)])}
    received = {}
    for offset in (-2, -1, 1, 2):
        pairs = [(i, i - offset) for i in range(groups) if 0 <= i - offset < groups]
        if pairs:
            received[(offset,)] = lax.ppermute(value, "grp", pairs)
    return received


def mixed(own, others, weights):
    total = weights[0] * own.astype(jnp.float32)
    for offsets, value in others.items():
        total = total + sum(weights[o] for o in offsets) * value.astype(jnp.float32)
    return total


PIECES = 4


def residual_kernel(
    z_size, part_ref, target_ref, out_ref, core_in, core_sum, y_in, y_sum, z_in, *sems
):
    (core_s, core_r, y_s, y_r, z_s, z_r, gz_s, gz_r, gy_s, gy_r, gc_s, gc_r) = sems
    me = lax.axis_index("blk")
    c = lax.rem(me, 2)
    y = lax.rem(lax.div(me, 2), 2)
    z = lax.div(me, 4)
    core_peer = z * 4 + y * 2 + (1 - c)
    y_peer = z * 4 + (1 - y) * 2 + c
    z_spots = [lax.rem(z + k, z_size) for k in range(1, z_size)]
    z_peers = [spot * 4 + y * 2 + c for spot in z_spots]
    width = target_ref.shape[-1] // PIECES
    columns = [pl.ds(q * width, width) for q in range(PIECES)]

    barrier = pltpu.get_barrier_semaphore()
    for peer in [core_peer, y_peer, *z_peers]:
        pl.semaphore_signal(barrier, inc=1, device_id={"blk": peer}, device_id_type=MESH)
    pl.semaphore_wait(barrier, z_size + 1)

    def send(src, dst, send_sem, recv_sem, peer):
        copy = pltpu.make_async_remote_copy(
            src_ref=src,
            dst_ref=dst,
            send_sem=send_sem,
            recv_sem=recv_sem,
            device_id={"blk": peer},
            device_id_type=MESH,
        )
        copy.start()
        return copy

    over_core = [
        send(part_ref.at[:, :, 1 - c, :, at], core_in.at[:, :, :, at], core_s.at[q], core_r.at[q], core_peer)
        for q, at in enumerate(columns)
    ]
    over_y = []
    for q, at in enumerate(columns):
        over_core[q].wait_recv()
        core_sum[:, :, :, at] = part_ref[:, :, c, :, at] + core_in[:, :, :, at]
        over_y.append(
            send(core_sum.at[:, 1 - y, :, at], y_in.at[:, :, at], y_s.at[q], y_r.at[q], y_peer)
        )
    over_z = []
    for q, at in enumerate(columns):
        over_y[q].wait_recv()
        y_sum[:, :, at] = core_sum[:, y, :, at] + y_in[:, :, at]
        over_z.append([
            send(y_sum.at[spot, :, at], z_in.at[k, :, at], z_s.at[q, k], z_r.at[q, k], z_peers[k])
            for k, spot in enumerate(z_spots)
        ])
    give_z = []
    for q, at in enumerate(columns):
        total = y_sum[z, :, at] - target_ref[:, at].astype(jnp.float32)
        for k, copy in enumerate(over_z[q]):
            copy.wait_recv()
            total = total + z_in[k, :, at]
        out_ref[z, y, c, :, at] = jnp.tanh(total).astype(jnp.bfloat16)
        mine = out_ref.at[z, y, c, :, at]
        give_z.append([
            send(mine, mine, gz_s.at[q, k], gz_r.at[q, k], peer) for k, peer in enumerate(z_peers)
        ])
    give_y = []
    for q, at in enumerate(columns):
        for copy in give_z[q]:
            copy.wait_recv()
        mine = out_ref.at[:, y, c, :, at]
        give_y.append(send(mine, mine, gy_s.at[q], gy_r.at[q], y_peer))
    give_core = []
    for q, at in enumerate(columns):
        give_y[q].wait_recv()
        mine = out_ref.at[:, :, c, :, at]
        give_core.append(send(mine, mine, gc_s.at[q], gc_r.at[q], core_peer))
    for copy in give_core:
        copy.wait_recv()
    for copy in [*over_core, *over_y, *sum(over_z, []), *sum(give_z, []), *give_y, *give_core]:
        copy.wait_send()


def residual(output, own_target, n, which):
    tokens, width = output.shape
    share, z_size = tokens // n, n // 4
    one = pltpu.SemaphoreType.DMA((PIECES,))
    many = pltpu.SemaphoreType.DMA((PIECES, z_size - 1))
    resid = pl.pallas_call(
        functools.partial(residual_kernel, z_size),
        out_shape=jax.ShapeDtypeStruct((z_size, 2, 2, share, width), jnp.bfloat16),
        in_specs=[pl.BlockSpec(memory_space=pltpu.VMEM)] * 2,
        out_specs=pl.BlockSpec(memory_space=pltpu.VMEM),
        scratch_shapes=[
            pltpu.VMEM((z_size, 2, share, width), jnp.float32),
            pltpu.VMEM((z_size, 2, share, width), jnp.float32),
            pltpu.VMEM((z_size, share, width), jnp.float32),
            pltpu.VMEM((z_size, share, width), jnp.float32),
            pltpu.VMEM((z_size - 1, share, width), jnp.float32),
            one, one, one, one, many, many, many, many, one, one, one, one,
        ],
        compiler_params=pltpu.CompilerParams(collective_id=which, has_side_effects=True),
        cost_estimate=pl.CostEstimate(flops=0, bytes_accessed=100 * tokens * width, transcendentals=0),
        name="residual",
    )(output.reshape(z_size, 2, 2, share, width), own_target)
    return resid.reshape(tokens, width)


def add_kernel(count, weights_ref, base_ref, *refs):
    out_ref = refs[-1]
    total = base_ref[...]
    for i, other in enumerate(refs[:count]):
        total = total + weights_ref[i] * other[...].astype(jnp.float32)
    out_ref[...] = total.astype(out_ref.dtype)


def add_others(base, others, weights, block):
    rows, width = base.shape
    count = others[0].shape[0] // block
    here = pl.BlockSpec((block, width), lambda i: (i, 0))
    return pl.pallas_call(
        functools.partial(add_kernel, len(others)),
        grid=(count,),
        out_shape=jax.ShapeDtypeStruct((rows, width), jnp.bfloat16),
        in_specs=[pl.BlockSpec(memory_space=pltpu.SMEM), here] + [here] * len(others),
        out_specs=here,
        compiler_params=pltpu.CompilerParams(dimension_semantics=("arbitrary",)),
        cost_estimate=pl.CostEstimate(
            flops=4 * count * block * width, bytes_accessed=8 * count * block * width, transcendentals=0
        ),
        name="add_others",
    )(weights, base, *others)


def body(params, tracker, hidden, target):
    groups, n = lax.axis_size("grp"), lax.axis_size("blk")
    weights = mix_weights(lax.axis_index("grp"), groups)
    tokens = hidden.shape[0]
    share = tokens // n
    own_target = lax.dynamic_slice_in_dim(target, lax.axis_index("blk") * share, share, 0)
    params, tracker = params[0], tracker[0]
    rows = params.shape[0]
    block = max(rows // 14 // 16, 1) * 16
    cuts = [(0, rows - 4 * block), (rows - 4 * block, rows - block), (rows - block, rows)]
    other_params = exchange(params, groups)
    other_tracker = [exchange(tracker[lo:hi], groups) for lo, hi in cuts]
    output_old = jnp.dot(hidden, params, preferred_element_type=jnp.float32)
    resid_old = residual(output_old, own_target, n, 0)
    params_next = (
        mixed(params, other_params, weights) - step_size * tracker.astype(jnp.float32)
    ).astype(jnp.bfloat16)
    output_new = jnp.dot(hidden, params_next, preferred_element_type=jnp.float32)
    resid_new = residual(output_new, own_target, n, 1)
    change = lax.dot_general(
        jnp.concatenate([hidden, -hidden], 0),
        jnp.concatenate([resid_new, resid_old], 0),
        (((0,), (0,)), ((), ())),
        preferred_element_type=jnp.float32,
    )
    base = weights[0] * tracker.astype(jnp.float32) + change / tokens
    late = lax.optimization_barrier([base[lo:hi] for lo, hi in cuts[1:]])
    gains = jnp.stack([sum(weights[o] for o in offsets) for offsets in other_tracker[0]])
    first = list(other_tracker[0].values())
    step = next(size for size in (4 * block, 2 * block, block) if first[0].shape[0] % size == 0)
    tracker_next = add_others(base, first, gains, step)
    for (lo, _), piece, received in zip(cuts[1:], late, other_tracker[1:]):
        for gain, value in zip(gains, received.values()):
            piece = piece + gain * value.astype(jnp.float32)
        tracker_next = lax.dynamic_update_slice(tracker_next, piece.astype(jnp.bfloat16), (lo, 0))
    return (params_next[None], tracker_next[None])


def solution(mesh):
    placed = (P("grp", "blk", None), P("grp", "blk", None), P("grp", "blk"), P("grp", None))
    return jax.shard_map(
        body,
        mesh=mesh,
        in_specs=placed,
        out_specs=(P("grp", "blk", None), P("grp", "blk", None)),
        check_vma=False,
    )
```

```python
import functools

import jax
import jax.numpy as jnp
from jax import lax
from jax.experimental import pallas as pl
from jax.experimental.pallas import tpu as pltpu
from jax.sharding import PartitionSpec as P

step_size = 0.05
MESH = pl.DeviceIdType.MESH


def mix_weights(position, groups):
    def has(spot):
        return ((spot >= 0) & (spot < groups)).astype(jnp.float32)

    def row(spot):
        a, b = has(spot - 1) / 3.0, has(spot + 1) / 3.0
        return a, 1.0 - a - b, b

    here, before, after = row(position), row(position - 1), row(position + 1)
    return {
        -2: here[0] * before[0],
        -1: here[0] * before[1] + here[1] * here[0],
        0: here[1] * here[1] + here[0] * before[2] + here[2] * after[0],
        1: here[2] * after[1] + here[1] * here[2],
        2: here[2] * after[2],
    }


def exchange(value, groups):
    if groups == 2:
        return {(-1, 1): lax.ppermute(value, "grp", [(0, 1), (1, 0)])}
    received = {}
    for offset in (-2, -1, 1, 2):
        pairs = [(i, i - offset) for i in range(groups) if 0 <= i - offset < groups]
        if pairs:
            received[(offset,)] = lax.ppermute(value, "grp", pairs)
    return received


def mixed(own, others, weights):
    total = weights[0] * own.astype(jnp.float32)
    for offsets, value in others.items():
        total = total + sum(weights[o] for o in offsets) * value.astype(jnp.float32)
    return total


PIECES = 4


def residual_kernel(
    z_size, part_ref, target_ref, out_ref, core_in, core_sum, y_in, y_sum, z_in, *sems
):
    (core_s, core_r, y_s, y_r, z_s, z_r, gz_s, gz_r, gy_s, gy_r, gc_s, gc_r) = sems
    me = lax.axis_index("blk")
    c = lax.rem(me, 2)
    y = lax.rem(lax.div(me, 2), 2)
    z = lax.div(me, 4)
    core_peer = z * 4 + y * 2 + (1 - c)
    y_peer = z * 4 + (1 - y) * 2 + c
    z_spots = [lax.rem(z + k, z_size) for k in range(1, z_size)]
    z_peers = [spot * 4 + y * 2 + c for spot in z_spots]
    width = target_ref.shape[-1] // PIECES
    columns = [pl.ds(q * width, width) for q in range(PIECES)]

    barrier = pltpu.get_barrier_semaphore()
    for peer in [core_peer, y_peer, *z_peers]:
        pl.semaphore_signal(barrier, inc=1, device_id={"blk": peer}, device_id_type=MESH)
    pl.semaphore_wait(barrier, z_size + 1)

    def send(src, dst, send_sem, recv_sem, peer):
        copy = pltpu.make_async_remote_copy(
            src_ref=src,
            dst_ref=dst,
            send_sem=send_sem,
            recv_sem=recv_sem,
            device_id={"blk": peer},
            device_id_type=MESH,
        )
        copy.start()
        return copy

    over_core = [
        send(part_ref.at[:, :, 1 - c, :, at], core_in.at[:, :, :, at], core_s.at[q], core_r.at[q], core_peer)
        for q, at in enumerate(columns)
    ]
    over_y = []
    for q, at in enumerate(columns):
        over_core[q].wait_recv()
        core_sum[:, :, :, at] = part_ref[:, :, c, :, at] + core_in[:, :, :, at]
        over_y.append(
            send(core_sum.at[:, 1 - y, :, at], y_in.at[:, :, at], y_s.at[q], y_r.at[q], y_peer)
        )
    over_z = []
    for q, at in enumerate(columns):
        over_y[q].wait_recv()
        y_sum[:, :, at] = core_sum[:, y, :, at] + y_in[:, :, at]
        over_z.append([
            send(y_sum.at[spot, :, at], z_in.at[k, :, at], z_s.at[q, k], z_r.at[q, k], z_peers[k])
            for k, spot in enumerate(z_spots)
        ])
    give_z = []
    for q, at in enumerate(columns):
        total = y_sum[z, :, at] - target_ref[:, at].astype(jnp.float32)
        for k, copy in enumerate(over_z[q]):
            copy.wait_recv()
            total = total + z_in[k, :, at]
        out_ref[z, y, c, :, at] = jnp.tanh(total).astype(jnp.bfloat16)
        mine = out_ref.at[z, y, c, :, at]
        give_z.append([
            send(mine, mine, gz_s.at[q, k], gz_r.at[q, k], peer) for k, peer in enumerate(z_peers)
        ])
    give_y = []
    for q, at in enumerate(columns):
        for copy in give_z[q]:
            copy.wait_recv()
        mine = out_ref.at[:, y, c, :, at]
        give_y.append(send(mine, mine, gy_s.at[q], gy_r.at[q], y_peer))
    give_core = []
    for q, at in enumerate(columns):
        give_y[q].wait_recv()
        mine = out_ref.at[:, :, c, :, at]
        give_core.append(send(mine, mine, gc_s.at[q], gc_r.at[q], core_peer))
    for copy in give_core:
        copy.wait_recv()
    for copy in [*over_core, *over_y, *sum(over_z, []), *sum(give_z, []), *give_y, *give_core]:
        copy.wait_send()


def residual(output, own_target, n, which):
    tokens, width = output.shape
    share, z_size = tokens // n, n // 4
    one = pltpu.SemaphoreType.DMA((PIECES,))
    many = pltpu.SemaphoreType.DMA((PIECES, z_size - 1))
    resid = pl.pallas_call(
        functools.partial(residual_kernel, z_size),
        out_shape=jax.ShapeDtypeStruct((z_size, 2, 2, share, width), jnp.bfloat16),
        in_specs=[pl.BlockSpec(memory_space=pltpu.VMEM)] * 2,
        out_specs=pl.BlockSpec(memory_space=pltpu.VMEM),
        scratch_shapes=[
            pltpu.VMEM((z_size, 2, share, width), jnp.float32),
            pltpu.VMEM((z_size, 2, share, width), jnp.float32),
            pltpu.VMEM((z_size, share, width), jnp.float32),
            pltpu.VMEM((z_size, share, width), jnp.float32),
            pltpu.VMEM((z_size - 1, share, width), jnp.float32),
            one, one, one, one, many, many, many, many, one, one, one, one,
        ],
        compiler_params=pltpu.CompilerParams(collective_id=which, has_side_effects=True),
        cost_estimate=pl.CostEstimate(flops=0, bytes_accessed=100 * tokens * width, transcendentals=0),
        name="residual",
    )(output.reshape(z_size, 2, 2, share, width), own_target)
    return resid.reshape(tokens, width)


def add_kernel(count, weights_ref, base_ref, *refs):
    out_ref = refs[-1]
    total = base_ref[...]
    for i, other in enumerate(refs[:count]):
        total = total + weights_ref[i] * other[...].astype(jnp.float32)
    out_ref[...] = total.astype(out_ref.dtype)


def add_others(base, others, weights, block):
    rows, width = base.shape
    count = others[0].shape[0] // block
    here = pl.BlockSpec((block, width), lambda i: (i, 0))
    return pl.pallas_call(
        functools.partial(add_kernel, len(others)),
        grid=(count,),
        out_shape=jax.ShapeDtypeStruct((rows, width), jnp.bfloat16),
        in_specs=[pl.BlockSpec(memory_space=pltpu.SMEM), here] + [here] * len(others),
        out_specs=here,
        compiler_params=pltpu.CompilerParams(dimension_semantics=("arbitrary",)),
        cost_estimate=pl.CostEstimate(
            flops=4 * count * block * width, bytes_accessed=8 * count * block * width, transcendentals=0
        ),
        name="add_others",
    )(weights, base, *others)


def body(params, tracker, hidden, target):
    groups, n = lax.axis_size("grp"), lax.axis_size("blk")
    weights = mix_weights(lax.axis_index("grp"), groups)
    tokens = hidden.shape[0]
    share = tokens // n
    own_target = lax.dynamic_slice_in_dim(target, lax.axis_index("blk") * share, share, 0)
    params, tracker = params[0], tracker[0]
    rows = params.shape[0]
    block = 16
    cuts = [(0, rows * 5 // 7 // 16 * 16), (rows * 5 // 7 // 16 * 16, rows - block), (rows - block, rows)]
    other_params = exchange(params, groups)
    other_tracker = [exchange(tracker[lo:hi], groups) for lo, hi in cuts]
    output_old = jnp.dot(hidden, params, preferred_element_type=jnp.float32)
    resid_old = residual(output_old, own_target, n, 0)
    params_next = (
        mixed(params, other_params, weights) - step_size * tracker.astype(jnp.float32)
    ).astype(jnp.bfloat16)
    output_new = jnp.dot(hidden, params_next, preferred_element_type=jnp.float32)
    resid_new = residual(output_new, own_target, n, 1)
    change = lax.dot_general(
        jnp.concatenate([hidden, -hidden], 0),
        jnp.concatenate([resid_new, resid_old], 0),
        (((0,), (0,)), ((), ())),
        preferred_element_type=jnp.float32,
    )
    base = weights[0] * tracker.astype(jnp.float32) + change / tokens
    late = lax.optimization_barrier([base[lo:hi] for lo, hi in cuts[1:]])
    gains = jnp.stack([sum(weights[o] for o in offsets) for offsets in other_tracker[0]])
    first = list(other_tracker[0].values())
    step = next(size for size in (10 * block, 4 * block, block) if first[0].shape[0] % size == 0)
    tracker_next = add_others(base, first, gains, step)
    for (lo, _), piece, received in zip(cuts[1:], late, other_tracker[1:]):
        for gain, value in zip(gains, received.values()):
            piece = piece + gain * value.astype(jnp.float32)
        tracker_next = lax.dynamic_update_slice(tracker_next, piece.astype(jnp.bfloat16), (lo, 0))
    return (params_next[None], tracker_next[None])


def solution(mesh):
    placed = (P("grp", "blk", None), P("grp", "blk", None), P("grp", "blk"), P("grp", None))
    return jax.shard_map(
        body,
        mesh=mesh,
        in_specs=placed,
        out_specs=(P("grp", "blk", None), P("grp", "blk", None)),
        check_vma=False,
    )
```
